128 devices in a mesh: dp: 1, sp: 128 (over z, y, x, core).
Axes of the slice: x: 4, y: 4, z: 4, core: 2. Of those that a mesh axis runs over, the one named last changes fastest.
Arguments:
- signal: bfloat16 [131072, 1024], P(('dp', 'sp'))
- w_first: bfloat16 [11, 2048, 2, 64, 64], P(None, 'sp')
- w_second: bfloat16 [11, 2048, 2, 64, 64], P(None, 'sp')
Outputs:
- output: bfloat16 [131072, 1024], P(('dp', 'sp'))
All inputs are finite; a program needn't handle non-finite values.
Results may differ from the reference program's by a relative error of at most 0.02.
Values are sent between devices in bfloat16 or wider.
A program may use at most 1 GiB of HBM per device.

```python
import jax
import jax.numpy as jnp
import math
from jax import lax

SEQ_LEN = 131072
CHANNELS = 1024
BLOCK_SIZE = 64

NUM_BLOCKS = SEQ_LEN // BLOCK_SIZE
STAGES = int(math.log2(NUM_BLOCKS))


def setup_inputs(seed: int = 0, part: int = 0) -> dict:
    key_signal = jax.random.fold_in(jax.random.key(seed + 1), part)
    key_first = jax.random.key(seed + 2)
    key_second = jax.random.key(seed + 3)
    w_shape = (STAGES, NUM_BLOCKS, 2, BLOCK_SIZE, BLOCK_SIZE)
    w_scale = (2 * BLOCK_SIZE) ** -0.5
    signal = jax.random.normal(key_signal, (SEQ_LEN, CHANNELS), jnp.float32)
    w_first = jax.random.normal(key_first, w_shape, jnp.float32) * w_scale
    w_second = jax.random.normal(key_second, w_shape, jnp.float32) * w_scale
    return {"signal": signal.astype(jnp.bfloat16), "w_first": w_first.astype(jnp.bfloat16), "w_second": w_second.astype(jnp.bfloat16)}


def butterfly_stage(act_blocks, weights, distance):
    grouped = act_blocks.reshape(NUM_BLOCKS // (2 * distance), 2, distance, BLOCK_SIZE, act_blocks.shape[2])
    partner = grouped[:, ::-1].reshape(act_blocks.shape)
    paired = jnp.stack([act_blocks, partner], axis=1).astype(jnp.float32)
    mixed = jnp.einsum("ltij,ltjc->lic", weights.astype(jnp.float32), paired)
    return mixed.astype(jnp.bfloat16)


def apply_map(act_blocks, weights, distances):
    for stage, distance in enumerate(distances):
        act_blocks = butterfly_stage(act_blocks, weights[stage], distance)
    return act_blocks


def reference(signal, w_first, w_second):
    col_width = min(CHANNELS, 128)
    col_groups = CHANNELS // col_width
    grouped = signal.reshape(NUM_BLOCKS, BLOCK_SIZE, col_groups, col_width).transpose(2, 0, 1, 3)
    dist_down = [2 ** (STAGES - 1 - level) for level in range(STAGES)]
    dist_up = [2 ** level for level in range(STAGES)]

    def one_group(act_blocks):
        hidden = apply_map(act_blocks, w_first, dist_down)
        hidden = jax.nn.gelu(hidden.astype(jnp.float32), approximate=False).astype(jnp.bfloat16)
        return apply_map(hidden, w_second, dist_up)

    mapped = lax.map(one_group, grouped)
    return mapped.transpose(1, 2, 0, 3).reshape(SEQ_LEN, CHANNELS)
```

```python
import functools

import jax
import jax.numpy as jnp
from jax import lax
from jax.experimental import pallas as pl
from jax.experimental.pallas import tpu as pltpu
from jax.sharding import PartitionSpec as P

MESH = pl.DeviceIdType.MESH

LANES = 128
BLOCK = 64
LOCAL = 16
SUB = 8
A_DIST = (8, 4, 2, 1)
B_DIST = (8, 4, 2)
N_DIST = (8, 4, 2, 1)
UP1, UP2, UP3, DOWN1, DOWN2, DOWN3 = range(6)


def gelu(x):
    return 0.5 * x * (1.0 + lax.erf(x * (0.5**0.5)))


def run_stages(buf, c, weights, stage0, dists, last=None):
    for step, dist in enumerate(dists):
        for low in range(LOCAL):
            if low & dist:
                continue
            high = low + dist
            act = jnp.concatenate([buf[c, low], buf[c, high]], axis=0)
            mat = jnp.concatenate([weights[stage0 + step, low], weights[stage0 + step, high]], axis=0)
            mixed = jnp.dot(mat, act, preferred_element_type=jnp.float32)
            if last is not None and step == len(dists) - 1:
                mixed = last(mixed.astype(jnp.bfloat16).astype(jnp.float32))
            mixed = mixed.astype(jnp.bfloat16)
            buf[c, low] = mixed[:BLOCK]
            buf[c, high] = mixed[BLOCK:]


def kernel(
    chunks,
    sig, w1, w2, out,
    inb, a1, b1, nb, b2, a2, ob,
    raw1, raw2, send_a, send_b, wa, wb, wn,
    in_sem, raw_sem, move_send, move_recv, wa_send, wa_recv, wb_send, wb_recv, out_sem,
):
    me = lax.axis_index("sp")
    zy = me // SUB
    xc = lax.rem(me, SUB)
    twist = 2 * (xc ^ 1)
    half = zy // 2
    own_l = zy ^ twist
    own_g = xc ^ half

    def device(zy_, xc_):
        return {"sp": zy_ * SUB + xc_}

    def remote(src, dst, send, recv, target):
        return pltpu.make_async_remote_copy(
            src_ref=src, dst_ref=dst, send_sem=send, recv_sem=recv, device_id=target, device_id_type=MESH
        )

    def in_copy(c):
        return pltpu.make_async_copy(sig.at[:, :, pl.ds(c * LANES, LANES)], inb.at[c], in_sem.at[c])

    def raw_copy(which, s):
        src, dst = ((w1, raw1), (w2, raw2))[which]
        return pltpu.make_async_copy(src.at[s], dst.at[s], raw_sem.at[which, s])

    def out_copy(c):
        return pltpu.make_async_copy(ob.at[c], out.at[:, :, pl.ds(c * LANES, LANES)], out_sem.at[c])


    def send_up1(c):
        def one(i, _):
            to = zy ^ i
            remote(
                inb.at[c, to ^ twist], a1.at[c, zy], move_send.at[UP1, c], move_recv.at[UP1, c], device(to, xc)
            ).start()
            return 0

        lax.fori_loop(1, LOCAL, one, 0)
        a1[c, zy] = inb[c, own_l]

    def send_up2(c):
        def one(i, _):
            q = zy ^ i
            remote(
                a1.at[c, q], b1.at[c, 2 * xc + lax.rem(own_l, 2)], move_send.at[UP2, c], move_recv.at[UP2, c],
                device(q, (own_l // 2) ^ (q // 2)),
            ).start()
            return 0

        lax.fori_loop(0, LOCAL, one, 0)

    def send_up3(c):
        def one(i, _):
            t = xc ^ i
            remote(
                b1.at[c, pl.ds(2 * t, 2)], nb.at[c, pl.ds(2 * own_g, 2)], move_send.at[UP3, c], move_recv.at[UP3, c],
                device(zy, t),
            ).start()
            return 0

        lax.fori_loop(1, SUB, one, 0)
        nb[c, pl.ds(2 * own_g, 2)] = b1[c, pl.ds(2 * xc, 2)]

    def send_down1(c):
        def one(i, _):
            to = xc ^ i
            remote(
                nb.at[c, pl.ds(2 * (to ^ half), 2)], b2.at[c, pl.ds(2 * xc, 2)], move_send.at[DOWN1, c],
                move_recv.at[DOWN1, c], device(zy, to),
            ).start()
            return 0

        lax.fori_loop(1, SUB, one, 0)
        b2[c, pl.ds(2 * xc, 2)] = nb[c, pl.ds(2 * own_g, 2)]

    def send_down2(c):
        def one(i, _):
            slot = i
            t = slot // 2
            to = (2 * own_g + lax.rem(slot, 2)) ^ (2 * (t ^ 1))
            remote(
                b2.at[c, slot], a2.at[c, zy], move_send.at[DOWN2, c], move_recv.at[DOWN2, c], device(to, t)
            ).start()
            return 0

        lax.fori_loop(0, LOCAL, one, 0)

    def send_down3(c):
        def one(i, _):
            q = zy ^ i
            remote(
                a2.at[c, q], ob.at[c, own_l], move_send.at[DOWN3, c], move_recv.at[DOWN3, c], device(q, xc)
            ).start()
            return 0

        lax.fori_loop(1, LOCAL, one, 0)
        ob[c, own_l] = a2[c, zy]

    remote_blocks = {UP1: 15, UP2: 16, UP3: 14, DOWN1: 14, DOWN2: 16, DOWN3: 15}

    def arrived(move, buf, c):
        n = remote_blocks[move]
        pltpu.make_async_copy(buf.at[c, pl.ds(0, n)], buf.at[c, pl.ds(0, n)], move_recv.at[move, c]).wait()

    def drained(move, buf, c):
        n = remote_blocks[move]
        pltpu.make_async_copy(buf.at[c, pl.ds(0, n)], buf.at[c, pl.ds(0, n)], move_send.at[move, c]).wait()


    def side_by_side(raw, s, l, bit):
        return jnp.concatenate([raw[s, l, bit], raw[s, l, 1 - bit]], axis=1)

    def send_wa(which, s, bit):
        raw = (raw1, raw2)[which]
        raw_s = s if which == 0 else 7 + s
        raw_copy(which, raw_s).wait()
        slot = 4 * which + s

        def build(l, _):
            send_a[slot, l] = side_by_side(raw, raw_s, l, bit)
            return 0

        lax.fori_loop(0, LOCAL, build, 0, unroll=4)

        def one(i, _):
            to = zy ^ i
            remote(
                send_a.at[slot, to ^ twist], wa.at[slot, zy], wa_send.at[slot], wa_recv.at[slot], device(to, xc)
            ).start()
            return 0

        lax.fori_loop(1, LOCAL, one, 0)
        wa[slot, zy] = send_a[slot, own_l]

    def send_wb(which, s, bit):
        raw = (raw1, raw2)[which]
        raw_copy(which, 4 + s).wait()
        slot = 3 * which + s

        def build(l, _):
            send_b[slot, l] = side_by_side(raw, 4 + s, l, bit)
            return 0

        lax.fori_loop(0, LOCAL, build, 0, unroll=4)

        def one(i, _):
            to = xc ^ i
            remote(
                send_b.at[slot, pl.ds(2 * (to ^ half), 2)], wb.at[slot, pl.ds(2 * xc, 2)], wb_send.at[slot],
                wb_recv.at[slot], device(zy, to),
            ).start()
            return 0

        lax.fori_loop(1, SUB, one, 0)
        wb[slot, pl.ds(2 * xc, 2)] = send_b[slot, pl.ds(2 * own_g, 2)]

    def build_wn(which, s, dist):
        raw = (raw1, raw2)[which]
        raw_s = 7 + s if which == 0 else s
        raw_copy(which, raw_s).wait()

        def build(l, _):
            wn[4 * which + s, l] = side_by_side(raw, raw_s, l, lax.rem(l // dist, 2))
            return 0

        lax.fori_loop(0, LOCAL, build, 0, unroll=4)

    def wa_arrived(slot, sem):
        pltpu.make_async_copy(wa.at[slot, pl.ds(0, 15)], wa.at[slot, pl.ds(0, 15)], sem.at[slot]).wait()

    def wb_arrived(slot, sem):
        pltpu.make_async_copy(wb.at[slot, pl.ds(0, 14)], wb.at[slot, pl.ds(0, 14)], sem.at[slot]).wait()


    in_copy(0).start()
    for s in range(4):
        raw_copy(0, s).start()
    for c in range(1, chunks):
        in_copy(c).start()
    for s in range(4, 11):
        raw_copy(0, s).start()
    for s in range(11):
        raw_copy(1, s).start()

    in_copy(0).wait()
    send_up1(0)
    for s in range(4):
        send_wa(0, s, lax.rem(zy // A_DIST[s], 2))
    in_copy(1).wait()
    send_up1(1)
    for s in range(3):
        send_wb(0, s, lax.rem(xc // (B_DIST[s] // 2), 2))
    for s in range(4):
        build_wn(0, s, N_DIST[s])
    for s in range(4):
        build_wn(1, s, N_DIST[3 - s])
    for s in range(3):
        send_wb(1, s, lax.rem(xc // (B_DIST[2 - s] // 2), 2))


    def slot_body(t, _):
        @pl.when(t < chunks)
        def _():
            @pl.when(t == 0)
            def _():
                for s in range(4):
                    wa_arrived(s, wa_recv)

            arrived(UP1, a1, t)
            run_stages(a1, t, wa, 0, A_DIST)
            send_up2(t)

            @pl.when(t + 2 < chunks)
            def _():
                in_copy(t + 2).wait()
                send_up1(t + 2)

            @pl.when(t == 0)
            def _():
                for s in range(4):
                    send_wa(1, s, lax.rem(zy // A_DIST[3 - s], 2))

        c1 = t - 1

        @pl.when((c1 >= 0) & (c1 < chunks))
        def _():
            @pl.when(c1 == 0)
            def _():
                for s in range(3):
                    wb_arrived(s, wb_recv)

            arrived(UP2, b1, c1)
            run_stages(b1, c1, wb, 0, B_DIST)
            send_up3(c1)

        c2 = t - 2

        @pl.when((c2 >= 0) & (c2 < chunks))
        def _():
            arrived(UP3, nb, c2)
            run_stages(nb, c2, wn, 0, N_DIST, last=gelu)
            run_stages(nb, c2, wn, 4, N_DIST[::-1])
            send_down1(c2)

        c3 = t - 3

        @pl.when((c3 >= 0) & (c3 < chunks))
        def _():
            @pl.when(c3 == 0)
            def _():
                for s in range(3):
                    wb_arrived(3 + s, wb_recv)

            arrived(DOWN1, b2, c3)
            run_stages(b2, c3, wb, 3, B_DIST[::-1])
            send_down2(c3)

        c4 = t - 4

        @pl.when((c4 >= 0) & (c4 < chunks))
        def _():
            @pl.when(c4 == 0)
            def _():
                for s in range(4):
                    wa_arrived(4 + s, wa_recv)

            arrived(DOWN2, a2, c4)
            run_stages(a2, c4, wa, 4, A_DIST[::-1])
            send_down3(c4)

        c5 = t - 5

        @pl.when(c5 >= 0)
        def _():
            arrived(DOWN3, ob, c5)
            out_copy(c5).start()

        return 0

    lax.fori_loop(0, chunks + 5, slot_body, 0)

    def finish(c, _):
        out_copy(c).wait()
        drained(UP1, inb, c)
        drained(UP2, a1, c)
        drained(UP3, b1, c)
        drained(DOWN1, nb, c)
        drained(DOWN2, b2, c)
        drained(DOWN3, a2, c)
        return 0

    lax.fori_loop(0, chunks, finish, 0)
    for slot in range(8):
        wa_arrived(slot, wa_send)
    for slot in range(6):
        wb_arrived(slot, wb_send)


def solution(mesh):
    def device_program(signal, w_first, w_second):
        rows, columns = signal.shape
        stages = w_first.shape[0]
        chunks = columns // LANES
        bf16 = jnp.bfloat16
        moved = pltpu.VMEM((chunks, LOCAL, BLOCK, LANES), bf16)
        raw = pltpu.VMEM((stages, LOCAL, 2, BLOCK, BLOCK), bf16)

        def paired(n):
            return pltpu.VMEM((n, LOCAL, BLOCK, LANES), bf16)

        dma = pltpu.SemaphoreType.DMA
        hbm = pl.BlockSpec(memory_space=pl.ANY)
        result = pl.pallas_call(
            functools.partial(kernel, chunks),
            out_shape=jax.ShapeDtypeStruct((LOCAL, BLOCK, columns), bf16),
            in_specs=[hbm, hbm, hbm],
            out_specs=hbm,
            scratch_shapes=[moved] * 7
            + [raw, raw, paired(8), paired(6), paired(8), paired(6), paired(8)]
            + [
                dma((chunks,)),
                dma((2, stages)),
                dma((6, chunks)),
                dma((6, chunks)),
                dma((8,)),
                dma((8,)),
                dma((6,)),
                dma((6,)),
                dma((chunks,)),
            ],
            compiler_params=pltpu.CompilerParams(has_side_effects=True, vmem_limit_bytes=60 * 2**20),
        )(signal.reshape(LOCAL, BLOCK, columns), w_first, w_second)
        return result.reshape(rows, columns)

    row_spec = P(("dp", "sp"), None)
    weight_spec = P(None, "sp", None, None, None)
    return jax.shard_map(
        device_program, mesh=mesh, in_specs=(row_spec, weight_spec, weight_spec), out_specs=row_spec, check_vma=False
    )
```

```python
import functools

import jax
import jax.numpy as jnp
from jax import lax
from jax.experimental import pallas as pl
from jax.experimental.pallas import tpu as pltpu
from jax.sharding import PartitionSpec as P

MESH = pl.DeviceIdType.MESH

LANES = 128
BLOCK = 64
LOCAL = 16
SUB = 8
A_DIST = (8, 4, 2, 1)
B_DIST = (8, 4, 2)
N_DIST = (8, 4, 2, 1)
UP1, UP2, UP3, DOWN1, DOWN2, DOWN3 = range(6)
AT_A1, AT_B1, AT_N, AT_B2, AT_A2, AT_OUT = 0, 2, 4, 6, 8, 10
AHEAD = 3
AT_WA2 = 5


def swap(v):
    return lax.rem(v, 2) + 2 * (v // 4) + 4 * lax.rem(v // 2, 2)


def gelu(x):
    return 0.5 * x * (1.0 + lax.erf(x * (0.5**0.5)))


def run_stages(buf, c, weights, stage0, dists, last=None):
    for step, dist in enumerate(dists):
        for low in range(LOCAL):
            if low & dist:
                continue
            high = low + dist
            act = jnp.concatenate([buf[c, low], buf[c, high]], axis=0)
            mat = jnp.concatenate([weights[stage0 + step, low], weights[stage0 + step, high]], axis=0)
            mixed = jnp.dot(mat, act, preferred_element_type=jnp.float32)
            if last is not None and step == len(dists) - 1:
                mixed = last(mixed.astype(jnp.bfloat16).astype(jnp.float32))
            mixed = mixed.astype(jnp.bfloat16)
            buf[c, low] = mixed[:BLOCK]
            buf[c, high] = mixed[BLOCK:]


def kernel(
    chunks,
    sig, w1, w2, out,
    inb, a1, b1, nb, b2, a2, ob,
    raw1, raw2, send_a, send_b, wa, wb, wn,
    in_sem, raw_sem, move_send, move_recv, wa_send, wa_recv, wb_send, wb_recv, out_sem,
):
    me = lax.axis_index("sp")
    zy = me // SUB
    xc = lax.rem(me, SUB)
    twist = 2 * swap(xc ^ 7)
    half = zy // 2
    own_l = zy ^ twist
    own_h = swap(xc) ^ half

    def device(zy_, xc_):
        return {"sp": zy_ * SUB + xc_}

    def remote(src, dst, send, recv, target):
        return pltpu.make_async_remote_copy(
            src_ref=src, dst_ref=dst, send_sem=send, recv_sem=recv, device_id=target, device_id_type=MESH
        )

    def in_copy(c):
        return pltpu.make_async_copy(sig.at[:, :, pl.ds(c * LANES, LANES)], inb.at[c], in_sem.at[c])

    def raw_copy(which, s):
        src, dst = ((w1, raw1), (w2, raw2))[which]
        return pltpu.make_async_copy(src.at[s], dst.at[s], raw_sem.at[which, s])

    def out_copy(c):
        return pltpu.make_async_copy(ob.at[c], out.at[:, :, pl.ds(c * LANES, LANES)], out_sem.at[c])


    def send_up1(c):
        def one(i, _):
            to = zy ^ i
            remote(
                inb.at[c, to ^ twist], a1.at[c, zy], move_send.at[UP1, c], move_recv.at[UP1, c], device(to, xc)
            ).start()
            return 0

        lax.fori_loop(1, LOCAL, one, 0)
        a1[c, zy] = inb[c, own_l]

    def send_up2(c):
        def one(i, _):
            q = zy ^ i
            remote(
                a1.at[c, q], b1.at[c, 2 * xc + lax.rem(own_l, 2)], move_send.at[UP2, c], move_recv.at[UP2, c],
                device(q, swap((own_l // 2) ^ (q // 2))),
            ).start()
            return 0

        lax.fori_loop(0, LOCAL, one, 0)

    def send_up3(c):
        def one(i, _):
            t = xc ^ i
            remote(
                b1.at[c, pl.ds(2 * t, 2)], nb.at[c, pl.ds(2 * own_h, 2)], move_send.at[UP3, c], move_recv.at[UP3, c],
                device(zy, t),
            ).start()
            return 0

        lax.fori_loop(1, SUB, one, 0)
        nb[c, pl.ds(2 * own_h, 2)] = b1[c, pl.ds(2 * xc, 2)]

    def send_down1(c):
        def one(i, _):
            to = xc ^ i
            remote(
                nb.at[c, pl.ds(2 * (swap(to) ^ half), 2)], b2.at[c, pl.ds(2 * xc, 2)], move_send.at[DOWN1, c],
                move_recv.at[DOWN1, c], device(zy, to),
            ).start()
            return 0

        lax.fori_loop(1, SUB, one, 0)
        b2[c, pl.ds(2 * xc, 2)] = nb[c, pl.ds(2 * own_h, 2)]

    def send_down2(c):
        def one(i, _):
            t = xc ^ (i // 2)
            slot = 2 * t + lax.rem(i, 2)
            to = (2 * own_h + lax.rem(i, 2)) ^ (2 * swap(t ^ 7))
            remote(
                b2.at[c, slot], a2.at[c, zy], move_send.at[DOWN2, c], move_recv.at[DOWN2, c], device(to, t)
            ).start()
            return 0

        lax.fori_loop(0, LOCAL, one, 0)

    def send_down3(c):
        def one(i, _):
            q = zy ^ i
            remote(
                a2.at[c, q], ob.at[c, own_l], move_send.at[DOWN3, c], move_recv.at[DOWN3, c], device(q, xc)
            ).start()
            return 0

        lax.fori_loop(1, LOCAL, one, 0)
        ob[c, own_l] = a2[c, zy]

    remote_blocks = {UP1: 15, UP2: 16, UP3: 14, DOWN1: 14, DOWN2: 16, DOWN3: 15}

    def arrived(move, buf, c):
        n = remote_blocks[move]
        pltpu.make_async_copy(buf.at[c, pl.ds(0, n)], buf.at[c, pl.ds(0, n)], move_recv.at[move, c]).wait()

    def drained(move, buf, c):
        n = remote_blocks[move]
        pltpu.make_async_copy(buf.at[c, pl.ds(0, n)], buf.at[c, pl.ds(0, n)], move_send.at[move, c]).wait()


    def side_by_side(raw, s, l, bit):
        return jnp.concatenate([raw[s, l, bit], raw[s, l, 1 - bit]], axis=1)

    def build_wa(which, s, bit):
        raw = (raw1, raw2)[which]
        raw_s = s if which == 0 else 7 + s
        raw_copy(which, raw_s).wait()
        slot = 4 * which + s

        def build(l, _):
            send_a[slot, l] = side_by_side(raw, raw_s, l, bit)
            return 0

        lax.fori_loop(0, LOCAL, build, 0, unroll=4)

    def send_wa(which, s):
        slot = 4 * which + s

        def one(i, _):
            to = zy ^ i
            remote(
                send_a.at[slot, to ^ twist], wa.at[slot, zy], wa_send.at[slot], wa_recv.at[slot], device(to, xc)
            ).start()
            return 0

        lax.fori_loop(1, LOCAL, one, 0)
        wa[slot, zy] = send_a[slot, own_l]

    def send_wb(which, s, bit):
        raw = (raw1, raw2)[which]
        raw_copy(which, 4 + s).wait()
        slot = 3 * which + s

        def build(l, _):
            send_b[slot, l] = side_by_side(raw, 4 + s, l, bit)
            return 0

        lax.fori_loop(0, LOCAL, build, 0, unroll=4)

        def one(i, _):
            to = xc ^ i
            remote(
                send_b.at[slot, pl.ds(2 * (swap(to) ^ half), 2)], wb.at[slot, pl.ds(2 * xc, 2)], wb_send.at[slot],
                wb_recv.at[slot], device(zy, to),
            ).start()
            return 0

        lax.fori_loop(1, SUB, one, 0)
        wb[slot, pl.ds(2 * xc, 2)] = send_b[slot, pl.ds(2 * own_h, 2)]

    def build_wn(which, s, dist):
        raw = (raw1, raw2)[which]
        raw_s = 7 + s if which == 0 else s
        raw_copy(which, raw_s).wait()

        def build(l, _):
            wn[4 * which + s, l] = side_by_side(raw, raw_s, l, lax.rem(l // dist, 2))
            return 0

        lax.fori_loop(0, LOCAL, build, 0, unroll=4)

    def wa_arrived(slot, sem):
        pltpu.make_async_copy(wa.at[slot, pl.ds(0, 15)], wa.at[slot, pl.ds(0, 15)], sem.at[slot]).wait()

    def wb_arrived(slot, sem):
        pltpu.make_async_copy(wb.at[slot, pl.ds(0, 14)], wb.at[slot, pl.ds(0, 14)], sem.at[slot]).wait()


    in_copy(0).start()
    for s in range(4):
        raw_copy(0, s).start()
    for c in range(1, chunks):
        in_copy(c).start()
    for s in range(4, 11):
        raw_copy(0, s).start()
    for s in range(11):
        raw_copy(1, s).start()


    barrier = pltpu.get_barrier_semaphore()

    def greet(target):
        pl.semaphore_signal(barrier, inc=1, device_id=target, device_id_type=MESH)

    def greet_zy(i, _):
        greet(device(zy ^ i, xc))
        return 0

    def greet_xc(i, _):
        greet(device(zy, xc ^ i))
        return 0

    def greet_all(q, _):
        greet(device(q, swap((own_l // 2) ^ (q // 2))))
        t = q // 2
        greet(device((2 * own_h + lax.rem(q, 2)) ^ (2 * swap(t ^ 7)), t))
        return 0

    lax.fori_loop(1, LOCAL, greet_zy, 0)
    lax.fori_loop(1, SUB, greet_xc, 0)
    lax.fori_loop(0, LOCAL, greet_all, 0)
    for s in range(4):
        build_wa(0, s, lax.rem(zy // A_DIST[s], 2))
    in_copy(0).wait()
    pl.semaphore_wait(barrier, 15 + 7 + 32)

    send_up1(0)
    for s in range(4):
        send_wa(0, s)
    for c in range(1, AHEAD):
        in_copy(c).wait()
        send_up1(c)
    for s in range(3):
        send_wb(0, s, lax.rem(xc // (B_DIST[s] // 2), 2))
    for s in range(4):
        build_wn(0, s, N_DIST[s])
    for s in range(4):
        build_wn(1, s, N_DIST[3 - s])
    for s in range(3):
        send_wb(1, s, lax.rem(xc // (B_DIST[2 - s] // 2), 2))


    def at(c, body):
        pl.when((c >= 0) & (c < chunks))(body)

    def slot_body(t, _):
        def first_a():
            c = t - AT_A1

            @pl.when(c == 0)
            def _():
                for s in range(4):
                    wa_arrived(s, wa_recv)

            arrived(UP1, a1, c)
            run_stages(a1, c, wa, 0, A_DIST)
            send_up2(c)

        at(t - AT_A1, first_a)

        @pl.when(t + AHEAD < chunks)
        def _():
            in_copy(t + AHEAD).wait()
            send_up1(t + AHEAD)

        @pl.when(t == AT_WA2)
        def _():
            for s in range(4):
                build_wa(1, s, lax.rem(zy // A_DIST[3 - s], 2))
                send_wa(1, s)

        def first_b():
            c = t - AT_B1

            @pl.when(c == 0)
            def _():
                for s in range(3):
                    wb_arrived(s, wb_recv)

            arrived(UP2, b1, c)
            run_stages(b1, c, wb, 0, B_DIST)
            send_up3(c)

        at(t - AT_B1, first_b)

        def middle():
            c = t - AT_N
            arrived(UP3, nb, c)
            run_stages(nb, c, wn, 0, N_DIST, last=gelu)
            run_stages(nb, c, wn, 4, N_DIST[::-1])
            send_down1(c)

        at(t - AT_N, middle)

        def second_b():
            c = t - AT_B2

            @pl.when(c == 0)
            def _():
                for s in range(3):
                    wb_arrived(3 + s, wb_recv)

            arrived(DOWN1, b2, c)
            run_stages(b2, c, wb, 3, B_DIST[::-1])
            send_down2(c)

        at(t - AT_B2, second_b)

        def second_a():
            c = t - AT_A2

            @pl.when(c == 0)
            def _():
                for s in range(4):
                    wa_arrived(4 + s, wa_recv)

            arrived(DOWN2, a2, c)
            run_stages(a2, c, wa, 4, A_DIST[::-1])
            send_down3(c)

        at(t - AT_A2, second_a)

        def store():
            c = t - AT_OUT
            arrived(DOWN3, ob, c)
            out_copy(c).start()

        at(t - AT_OUT, store)
        return 0

    lax.fori_loop(0, chunks + AT_OUT, slot_body, 0)

    def finish(c, _):
        out_copy(c).wait()
        drained(UP1, inb, c)
        drained(UP2, a1, c)
        drained(UP3, b1, c)
        drained(DOWN1, nb, c)
        drained(DOWN2, b2, c)
        drained(DOWN3, a2, c)
        return 0

    lax.fori_loop(0, chunks, finish, 0)
    for slot in range(8):
        wa_arrived(slot, wa_send)
    for slot in range(6):
        wb_arrived(slot, wb_send)


def solution(mesh):
    def device_program(signal, w_first, w_second):
        rows, columns = signal.shape
        stages = w_first.shape[0]
        chunks = columns // LANES
        bf16 = jnp.bfloat16
        moved = pltpu.VMEM((chunks, LOCAL, BLOCK, LANES), bf16)
        raw = pltpu.VMEM((stages, LOCAL, 2, BLOCK, BLOCK), bf16)

        def paired(n):
            return pltpu.VMEM((n, LOCAL, BLOCK, LANES), bf16)

        dma = pltpu.SemaphoreType.DMA
        hbm = pl.BlockSpec(memory_space=pl.ANY)
        result = pl.pallas_call(
            functools.partial(kernel, chunks),
            out_shape=jax.ShapeDtypeStruct((LOCAL, BLOCK, columns), bf16),
            in_specs=[hbm, hbm, hbm],
            out_specs=hbm,
            scratch_shapes=[moved] * 7
            + [raw, raw, paired(8), paired(6), paired(8), paired(6), paired(8)]
            + [
                dma((chunks,)),
                dma((2, stages)),
                dma((6, chunks)),
                dma((6, chunks)),
                dma((8,)),
                dma((8,)),
                dma((6,)),
                dma((6,)),
                dma((chunks,)),
            ],
            compiler_params=pltpu.CompilerParams(
                collective_id=0, has_side_effects=True, vmem_limit_bytes=60 * 2**20
            ),
        )(signal.reshape(LOCAL, BLOCK, columns), w_first, w_second)
        return result.reshape(rows, columns)

    row_spec = P(("dp", "sp"), None)
    weight_spec = P(None, "sp", None, None, None)
    return jax.shard_map(
        device_program, mesh=mesh, in_specs=(row_spec, weight_spec, weight_spec), out_specs=row_spec, check_vma=False
    )
```

```python
import functools

import jax
import jax.numpy as jnp
from jax import lax
from jax.experimental import pallas as pl
from jax.experimental.pallas import tpu as pltpu
from jax.sharding import PartitionSpec as P

MESH = pl.DeviceIdType.MESH

LANES = 128
BLOCK = 64
HALF = 32
LOCAL = 16
SUB = 8
A_DIST = (8, 4, 2, 1)
B_DIST = (8, 4, 2)
N_DIST = (8, 4, 2, 1)
UP1, UP2, UP3, DOWN1, DOWN2, DOWN3 = range(6)
AT_A1, AT_B1, AT_N, AT_B2, AT_A2, AT_OUT = 0, 2, 4, 6, 8, 10
AHEAD = 3
AT_WA2 = 5


def swap(v):
    return lax.rem(v, 2) + 2 * (v // 4) + 4 * lax.rem(v // 2, 2)


def gelu(x):
    return 0.5 * x * (1.0 + lax.erf(x * (0.5**0.5)))


def run_stages(buf, c, weights, stage0, dists, last=None):
    for step, dist in enumerate(dists):
        for low in range(LOCAL):
            if low & dist:
                continue
            high = low + dist
            act = jnp.concatenate([buf[c, low], buf[c, high]], axis=0)
            mat = jnp.concatenate([weights[stage0 + step, low], weights[stage0 + step, high]], axis=0)
            mixed = jnp.dot(mat, act, preferred_element_type=jnp.float32)
            if last is not None and step == len(dists) - 1:
                mixed = last(mixed.astype(jnp.bfloat16).astype(jnp.float32))
            mixed = mixed.astype(jnp.bfloat16)
            buf[c, low] = mixed[:BLOCK]
            buf[c, high] = mixed[BLOCK:]


def kernel(
    chunks,
    sig, w1, w2, ob,
    inb, a1, b1, nb, b2, a2,
    raw1, raw2, send_a, send_b, wa, wb, wn,
    in_sem, raw_sem, move_send, move_recv, wa_send, wa_recv, wb_send, wb_recv, out_sem,
):
    me = lax.axis_index("sp")
    zy = me // SUB
    xc = lax.rem(me, SUB)
    twist = 2 * swap(xc ^ 7)
    half = zy // 2
    own_l = zy ^ twist
    own_h = swap(xc) ^ half

    def device(zy_, xc_):
        return {"sp": zy_ * SUB + xc_}

    def remote(src, dst, send, recv, target):
        return pltpu.make_async_remote_copy(
            src_ref=src, dst_ref=dst, send_sem=send, recv_sem=recv, device_id=target, device_id_type=MESH
        )

    def in_copy(c):
        return pltpu.make_async_copy(sig.at[:, :, pl.ds(c * LANES, LANES)], inb.at[c], in_sem.at[c])

    def raw_copy(which, s):
        src, dst = ((w1, raw1), (w2, raw2))[which]
        return pltpu.make_async_copy(src.at[s], dst.at[s], raw_sem.at[which, s])

    def out_copy(c):
        return pltpu.make_async_copy(a2.at[c, zy], ob.at[c, own_l], out_sem.at[c])


    def send_up1(c):
        def one(i, _):
            to = zy ^ (1 + lax.rem(i, LOCAL - 1))
            rows = pl.ds((i // (LOCAL - 1)) * HALF, HALF)
            remote(
                inb.at[c, to ^ twist, rows], a1.at[c, zy, rows], move_send.at[UP1, c], move_recv.at[UP1, c],
                device(to, xc),
            ).start()
            return 0

        lax.fori_loop(0, 2 * (LOCAL - 1), one, 0)
        a1[c, zy] = inb[c, own_l]

    def send_up2(c):
        def one(i, _):
            q = zy ^ i
            remote(
                a1.at[c, q], b1.at[c, 2 * xc + lax.rem(own_l, 2)], move_send.at[UP2, c], move_recv.at[UP2, c],
                device(q, swap((own_l // 2) ^ (q // 2))),
            ).start()
            return 0

        lax.fori_loop(0, LOCAL, one, 0)

    def send_up3(c):
        def one(i, _):
            t = xc ^ i
            remote(
                b1.at[c, pl.ds(2 * t, 2)], nb.at[c, pl.ds(2 * own_h, 2)], move_send.at[UP3, c], move_recv.at[UP3, c],
                device(zy, t),
            ).start()
            return 0

        lax.fori_loop(1, SUB, one, 0)
        nb[c, pl.ds(2 * own_h, 2)] = b1[c, pl.ds(2 * xc, 2)]

    def send_down1(c):
        def one(i, _):
            to = xc ^ i
            remote(
                nb.at[c, pl.ds(2 * (swap(to) ^ half), 2)], b2.at[c, pl.ds(2 * xc, 2)], move_send.at[DOWN1, c],
                move_recv.at[DOWN1, c], device(zy, to),
            ).start()
            return 0

        lax.fori_loop(1, SUB, one, 0)
        b2[c, pl.ds(2 * xc, 2)] = nb[c, pl.ds(2 * own_h, 2)]

    def send_down2(c):
        def one(i, _):
            t = xc ^ (i // 2)
            slot = 2 * t + lax.rem(i, 2)
            to = (2 * own_h + lax.rem(i, 2)) ^ (2 * swap(t ^ 7))
            remote(
                b2.at[c, slot], a2.at[c, zy], move_send.at[DOWN2, c], move_recv.at[DOWN2, c], device(to, t)
            ).start()
            return 0

        lax.fori_loop(0, LOCAL, one, 0)

    def send_down3(c):
        def one(i, _):
            q = zy ^ (1 + lax.rem(i, LOCAL - 1))
            rows = pl.ds((i // (LOCAL - 1)) * HALF, HALF)
            remote(
                a2.at[c, q, rows], ob.at[c, own_l, rows], move_send.at[DOWN3, c], move_recv.at[DOWN3, c],
                device(q, xc),
            ).start()
            return 0

        lax.fori_loop(0, 2 * (LOCAL - 1), one, 0)
        out_copy(c).start()

    remote_blocks = {UP1: 15, UP2: 16, UP3: 14, DOWN1: 14, DOWN2: 16, DOWN3: 15}

    def arrived(move, buf, c):
        n = remote_blocks[move]
        pltpu.make_async_copy(buf.at[c, pl.ds(0, n)], buf.at[c, pl.ds(0, n)], move_recv.at[move, c]).wait()

    def drained(move, buf, c):
        n = remote_blocks[move]
        pltpu.make_async_copy(buf.at[c, pl.ds(0, n)], buf.at[c, pl.ds(0, n)], move_send.at[move, c]).wait()


    def side_by_side(raw, s, l, bit):
        return jnp.concatenate([raw[s, l, bit], raw[s, l, 1 - bit]], axis=1)

    def build_wa(which, s, bit):
        raw = (raw1, raw2)[which]
        raw_s = s if which == 0 else 7 + s
        raw_copy(which, raw_s).wait()
        slot = 4 * which + s

        def build(l, _):
            send_a[slot, l] = side_by_side(raw, raw_s, l, bit)
            return 0

        lax.fori_loop(0, LOCAL, build, 0, unroll=4)

    def send_wa(which, s):
        slot = 4 * which + s

        def one(i, _):
            to = zy ^ (1 + lax.rem(i, LOCAL - 1))
            rows = pl.ds((i // (LOCAL - 1)) * HALF, HALF)
            remote(
                send_a.at[slot, to ^ twist, rows], wa.at[slot, zy, rows], wa_send.at[slot], wa_recv.at[slot],
                device(to, xc),
            ).start()
            return 0

        lax.fori_loop(0, 2 * (LOCAL - 1), one, 0)
        wa[slot, zy] = send_a[slot, own_l]

    def send_wb(which, s, bit):
        raw = (raw1, raw2)[which]
        raw_copy(which, 4 + s).wait()
        slot = 3 * which + s

        def build(l, _):
            send_b[slot, l] = side_by_side(raw, 4 + s, l, bit)
            return 0

        lax.fori_loop(0, LOCAL, build, 0, unroll=4)

        def one(i, _):
            to = xc ^ i
            remote(
                send_b.at[slot, pl.ds(2 * (swap(to) ^ half), 2)], wb.at[slot, pl.ds(2 * xc, 2)], wb_send.at[slot],
                wb_recv.at[slot], device(zy, to),
            ).start()
            return 0

        lax.fori_loop(1, SUB, one, 0)
        wb[slot, pl.ds(2 * xc, 2)] = send_b[slot, pl.ds(2 * own_h, 2)]

    def build_wn(which, s, dist):
        raw = (raw1, raw2)[which]
        raw_s = 7 + s if which == 0 else s
        raw_copy(which, raw_s).wait()

        def build(l, _):
            wn[4 * which + s, l] = side_by_side(raw, raw_s, l, lax.rem(l // dist, 2))
            return 0

        lax.fori_loop(0, LOCAL, build, 0, unroll=4)

    def wa_arrived(slot, sem):
        pltpu.make_async_copy(wa.at[slot, pl.ds(0, 15)], wa.at[slot, pl.ds(0, 15)], sem.at[slot]).wait()

    def wb_arrived(slot, sem):
        pltpu.make_async_copy(wb.at[slot, pl.ds(0, 14)], wb.at[slot, pl.ds(0, 14)], sem.at[slot]).wait()


    in_copy(0).start()
    for s in range(4):
        raw_copy(0, s).start()
    for c in range(1, chunks):
        in_copy(c).start()
    for s in range(4, 11):
        raw_copy(0, s).start()
    for s in range(11):
        raw_copy(1, s).start()


    barrier = pltpu.get_barrier_semaphore()

    def greet(target):
        pl.semaphore_signal(barrier, inc=1, device_id=target, device_id_type=MESH)

    def greet_zy(i, _):
        greet(device(zy ^ i, xc))
        return 0

    def greet_xc(i, _):
        greet(device(zy, xc ^ i))
        return 0

    def greet_all(q, _):
        greet(device(q, swap((own_l // 2) ^ (q // 2))))
        t = q // 2
        greet(device((2 * own_h + lax.rem(q, 2)) ^ (2 * swap(t ^ 7)), t))
        return 0

    lax.fori_loop(1, LOCAL, greet_zy, 0)
    lax.fori_loop(1, SUB, greet_xc, 0)
    lax.fori_loop(0, LOCAL, greet_all, 0)
    for s in range(4):
        build_wa(0, s, lax.rem(zy // A_DIST[s], 2))
    in_copy(0).wait()
    pl.semaphore_wait(barrier, 15 + 7 + 32)

    send_up1(0)
    for s in range(4):
        send_wa(0, s)
    for c in range(1, AHEAD):
        in_copy(c).wait()
        send_up1(c)
    for s in range(3):
        send_wb(0, s, lax.rem(xc // (B_DIST[s] // 2), 2))
    for s in range(4):
        build_wn(0, s, N_DIST[s])
    for s in range(4):
        build_wn(1, s, N_DIST[3 - s])
    for s in range(3):
        send_wb(1, s, lax.rem(xc // (B_DIST[2 - s] // 2), 2))


    def at(c, body):
        pl.when((c >= 0) & (c < chunks))(body)

    def slot_body(t, _):
        def first_a():
            c = t - AT_A1

            @pl.when(c == 0)
            def _():
                for s in range(4):
                    wa_arrived(s, wa_recv)

            arrived(UP1, a1, c)
            run_stages(a1, c, wa, 0, A_DIST)
            send_up2(c)

        at(t - AT_A1, first_a)

        @pl.when(t + AHEAD < chunks)
        def _():
            in_copy(t + AHEAD).wait()
            send_up1(t + AHEAD)

        @pl.when(t == AT_WA2)
        def _():
            for s in range(4):
                build_wa(1, s, lax.rem(zy // A_DIST[3 - s], 2))
                send_wa(1, s)

        def first_b():
            c = t - AT_B1

            @pl.when(c == 0)
            def _():
                for s in range(3):
                    wb_arrived(s, wb_recv)

            arrived(UP2, b1, c)
            run_stages(b1, c, wb, 0, B_DIST)
            send_up3(c)

        at(t - AT_B1, first_b)

        def middle():
            c = t - AT_N
            arrived(UP3, nb, c)
            run_stages(nb, c, wn, 0, N_DIST, last=gelu)
            run_stages(nb, c, wn, 4, N_DIST[::-1])
            send_down1(c)

        at(t - AT_N, middle)

        def second_b():
            c = t - AT_B2

            @pl.when(c == 0)
            def _():
                for s in range(3):
                    wb_arrived(3 + s, wb_recv)

            arrived(DOWN1, b2, c)
            run_stages(b2, c, wb, 3, B_DIST[::-1])
            send_down2(c)

        at(t - AT_B2, second_b)

        def second_a():
            c = t - AT_A2

            @pl.when(c == 0)
            def _():
                for s in range(4):
                    wa_arrived(4 + s, wa_recv)

            arrived(DOWN2, a2, c)
            run_stages(a2, c, wa, 4, A_DIST[::-1])
            send_down3(c)

        at(t - AT_A2, second_a)

        def store():
            c = t - AT_OUT
            arrived(DOWN3, ob, c)

        at(t - AT_OUT, store)
        return 0

    lax.fori_loop(0, chunks + AT_OUT, slot_body, 0)

    def finish(c, _):
        out_copy(c).wait()
        drained(UP1, inb, c)
        drained(UP2, a1, c)
        drained(UP3, b1, c)
        drained(DOWN1, nb, c)
        drained(DOWN2, b2, c)
        drained(DOWN3, a2, c)
        return 0

    lax.fori_loop(0, chunks, finish, 0)
    for slot in range(8):
        wa_arrived(slot, wa_send)
    for slot in range(6):
        wb_arrived(slot, wb_send)


def gather_chunks(chunks, parts, out, buf, in_sem, out_sem):
    into = [pltpu.make_async_copy(parts.at[c], buf.at[c], in_sem.at[c]) for c in range(chunks)]
    onto = [
        pltpu.make_async_copy(buf.at[c], out.at[:, pl.ds(c * LANES, LANES)], out_sem.at[c]) for c in range(chunks)
    ]
    for copy in into:
        copy.start()
    for c in range(chunks):
        into[c].wait()
        onto[c].start()
    for copy in onto:
        copy.wait()


def solution(mesh):
    def device_program(signal, w_first, w_second):
        rows, columns = signal.shape
        stages = w_first.shape[0]
        chunks = columns // LANES
        bf16 = jnp.bfloat16
        moved = pltpu.VMEM((chunks, LOCAL, BLOCK, LANES), bf16)
        raw = pltpu.VMEM((stages, LOCAL, 2, BLOCK, BLOCK), bf16)

        def paired(n):
            return pltpu.VMEM((n, LOCAL, BLOCK, LANES), bf16)

        dma = pltpu.SemaphoreType.DMA
        hbm = pl.BlockSpec(memory_space=pl.ANY)
        result = pl.pallas_call(
            functools.partial(kernel, chunks),
            out_shape=jax.ShapeDtypeStruct((chunks, LOCAL, BLOCK, LANES), bf16),
            in_specs=[hbm, hbm, hbm],
            out_specs=hbm,
            scratch_shapes=[moved] * 6
            + [raw, raw, paired(8), paired(6), paired(8), paired(6), paired(8)]
            + [
                dma((chunks,)),
                dma((2, stages)),
                dma((6, chunks)),
                dma((6, chunks)),
                dma((8,)),
                dma((8,)),
                dma((6,)),
                dma((6,)),
                dma((chunks,)),
            ],
            compiler_params=pltpu.CompilerParams(
                collective_id=0, has_side_effects=True, vmem_limit_bytes=60 * 2**20
            ),
        )(signal.reshape(LOCAL, BLOCK, columns), w_first, w_second)
        return pl.pallas_call(
            functools.partial(gather_chunks, chunks),
            out_shape=jax.ShapeDtypeStruct((rows, columns), bf16),
            in_specs=[hbm],
            out_specs=hbm,
            scratch_shapes=[pltpu.VMEM((chunks, rows, LANES), bf16), dma((chunks,)), dma((chunks,))],
            compiler_params=pltpu.CompilerParams(vmem_limit_bytes=60 * 2**20),
        )(result.reshape(chunks, rows, LANES))

    row_spec = P(("dp", "sp"), None)
    weight_spec = P(None, "sp", None, None, None)
    return jax.shard_map(
        device_program, mesh=mesh, in_specs=(row_spec, weight_spec, weight_spec), out_specs=row_spec, check_vma=False
    )
```

```python
import functools

import jax
import jax.numpy as jnp
from jax import lax
from jax.experimental import pallas as pl
from jax.experimental.pallas import tpu as pltpu
from jax.sharding import PartitionSpec as P

MESH = pl.DeviceIdType.MESH

LANES = 128
BLOCK = 64
HALF = 32
LOCAL = 16
SUB = 8
A_DIST = (8, 4, 2, 1)
B_DIST = (8, 4, 2)
N_DIST = (8, 4, 2, 1)
UP1, UP2, UP3, DOWN1, DOWN2, DOWN3 = range(6)
AT_A1, AT_B1, AT_N, AT_B2, AT_A2 = 0, 2, 4, 6, 8
AHEAD = 3
AT_WA2 = 3


def swap(v):
    return lax.rem(v, 2) + 2 * (v // 4) + 4 * lax.rem(v // 2, 2)


def spread(i):
    return (15 * lax.rem(i, 2)) ^ (5 * lax.rem(i // 2, 2)) ^ (3 * lax.rem(i // 4, 2)) ^ (i // 8)


def gelu(x):
    return 0.5 * x * (1.0 + lax.erf(x * (0.5**0.5)))


def run_stages(buf, c, weights, stage0, dists, last=None):
    for step, dist in enumerate(dists):
        for low in range(LOCAL):
            if low & dist:
                continue
            high = low + dist
            act = jnp.concatenate([buf[c, low], buf[c, high]], axis=0)
            mat = jnp.concatenate([weights[stage0 + step, low], weights[stage0 + step, high]], axis=0)
            mixed = jnp.dot(mat, act, preferred_element_type=jnp.float32)
            if last is not None and step == len(dists) - 1:
                mixed = last(mixed.astype(jnp.bfloat16).astype(jnp.float32))
            mixed = mixed.astype(jnp.bfloat16)
            buf[c, low] = mixed[:BLOCK]
            buf[c, high] = mixed[BLOCK:]


def kernel(
    chunks,
    sig, w1, w2, ob,
    inb, a1, b1, nb, b2, a2,
    raw1, raw2, send_a, send_b, wa, wb, wn,
    in_sem, raw_sem, move_send, move_recv, wa_send, wa_recv, wb_send, wb_recv, out_sem,
):
    me = lax.axis_index("sp")
    zy = me // SUB
    xc = lax.rem(me, SUB)
    twist = 2 * swap(xc ^ 7)
    half = zy // 2
    own_l = zy ^ twist
    own_h = swap(xc) ^ half

    def device(zy_, xc_):
        return {"sp": zy_ * SUB + xc_}

    def remote(src, dst, send, recv, target):
        return pltpu.make_async_remote_copy(
            src_ref=src, dst_ref=dst, send_sem=send, recv_sem=recv, device_id=target, device_id_type=MESH
        )

    def in_copy(c):
        return pltpu.make_async_copy(sig.at[:, :, pl.ds(c * LANES, LANES)], inb.at[c], in_sem.at[c])

    def raw_copy(which, s):
        src, dst = ((w1, raw1), (w2, raw2))[which]
        return pltpu.make_async_copy(src.at[s], dst.at[s], raw_sem.at[which, s])

    def own_copy(c):
        return pltpu.make_async_copy(a2.at[c, zy], ob.at[c, own_l], out_sem.at[c])


    def send_up1(c):
        def one(i, _):
            to = zy ^ (1 + lax.rem(i, LOCAL - 1))
            rows = pl.ds((i // (LOCAL - 1)) * HALF, HALF)
            remote(
                inb.at[c, to ^ twist, rows], a1.at[c, zy, rows], move_send.at[UP1, c], move_recv.at[UP1, c],
                device(to, xc),
            ).start()
            return 0

        lax.fori_loop(0, 2 * (LOCAL - 1), one, 0)
        a1[c, zy] = inb[c, own_l]

    def send_up2(c):
        def one(i, _):
            q = zy ^ spread(lax.rem(i, LOCAL))
            rows = pl.ds((i // LOCAL) * HALF, HALF)
            remote(
                a1.at[c, q, rows], b1.at[c, 2 * xc + lax.rem(own_l, 2), rows], move_send.at[UP2, c],
                move_recv.at[UP2, c], device(q, swap((own_l // 2) ^ (q // 2))),
            ).start()
            return 0

        lax.fori_loop(0, 2 * LOCAL, one, 0)

    def send_up3(c):
        def one(i, _):
            t = xc ^ i
            remote(
                b1.at[c, pl.ds(2 * t, 2)], nb.at[c, pl.ds(2 * own_h, 2)], move_send.at[UP3, c], move_recv.at[UP3, c],
                device(zy, t),
            ).start()
            return 0

        lax.fori_loop(1, SUB, one, 0)
        nb[c, pl.ds(2 * own_h, 2)] = b1[c, pl.ds(2 * xc, 2)]

    def send_down1(c):
        def one(i, _):
            to = xc ^ i
            remote(
                nb.at[c, pl.ds(2 * (swap(to) ^ half), 2)], b2.at[c, pl.ds(2 * xc, 2)], move_send.at[DOWN1, c],
                move_recv.at[DOWN1, c], device(zy, to),
            ).start()
            return 0

        lax.fori_loop(1, SUB, one, 0)
        b2[c, pl.ds(2 * xc, 2)] = nb[c, pl.ds(2 * own_h, 2)]

    def send_down2(c):
        def one(i, _):
            step = spread(lax.rem(i, LOCAL))
            to, t = zy ^ step, xc ^ swap(step // 2) ^ 7
            rows = pl.ds((i // LOCAL) * HALF, HALF)
            remote(
                b2.at[c, 2 * t + lax.rem(to, 2), rows], a2.at[c, zy, rows], move_send.at[DOWN2, c],
                move_recv.at[DOWN2, c], device(to, t),
            ).start()
            return 0

        lax.fori_loop(0, 2 * LOCAL, one, 0)

    def send_down3(c):
        def one(i, _):
            q = zy ^ (1 + lax.rem(i, LOCAL - 1))
            rows = pl.ds((i // (LOCAL - 1)) * HALF, HALF)
            remote(
                a2.at[c, q, rows], ob.at[c, own_l, rows], move_send.at[DOWN3, c], move_recv.at[DOWN3, c],
                device(q, xc),
            ).start()
            return 0

        lax.fori_loop(0, 2 * (LOCAL - 1), one, 0)
        own_copy(c).start()

    remote_blocks = {UP1: 15, UP2: 16, UP3: 14, DOWN1: 14, DOWN2: 16, DOWN3: 15}

    def arrived(move, buf, c):
        n = remote_blocks[move]
        pltpu.make_async_copy(buf.at[c, pl.ds(0, n)], buf.at[c, pl.ds(0, n)], move_recv.at[move, c]).wait()

    def drained(move, buf, c):
        n = remote_blocks[move]
        pltpu.make_async_copy(buf.at[c, pl.ds(0, n)], buf.at[c, pl.ds(0, n)], move_send.at[move, c]).wait()


    def side_by_side(raw, s, l, bit):
        return jnp.concatenate([raw[s, l, bit], raw[s, l, 1 - bit]], axis=1)

    def build_wa(which, s, bit):
        raw = (raw1, raw2)[which]
        raw_s = s if which == 0 else 7 + s
        raw_copy(which, raw_s).wait()
        slot = 4 * which + s

        def build(l, _):
            send_a[slot, l] = side_by_side(raw, raw_s, l, bit)
            return 0

        lax.fori_loop(0, LOCAL, build, 0, unroll=4)

    def send_wa(which, s):
        slot = 4 * which + s

        def one(i, _):
            to = zy ^ (1 + lax.rem(i, LOCAL - 1))
            rows = pl.ds((i // (LOCAL - 1)) * HALF, HALF)
            remote(
                send_a.at[slot, to ^ twist, rows], wa.at[slot, zy, rows], wa_send.at[slot], wa_recv.at[slot],
                device(to, xc),
            ).start()
            return 0

        lax.fori_loop(0, 2 * (LOCAL - 1), one, 0)
        wa[slot, zy] = send_a[slot, own_l]

    def send_wb(which, s, bit):
        raw = (raw1, raw2)[which]
        raw_copy(which, 4 + s).wait()
        slot = 3 * which + s

        def build(l, _):
            send_b[slot, l] = side_by_side(raw, 4 + s, l, bit)
            return 0

        lax.fori_loop(0, LOCAL, build, 0, unroll=4)

        def one(i, _):
            to = xc ^ i
            remote(
                send_b.at[slot, pl.ds(2 * (swap(to) ^ half), 2)], wb.at[slot, pl.ds(2 * xc, 2)], wb_send.at[slot],
                wb_recv.at[slot], device(zy, to),
            ).start()
            return 0

        lax.fori_loop(1, SUB, one, 0)
        wb[slot, pl.ds(2 * xc, 2)] = send_b[slot, pl.ds(2 * own_h, 2)]

    def build_wn(which, s, dist):
        raw = (raw1, raw2)[which]
        raw_s = 7 + s if which == 0 else s
        raw_copy(which, raw_s).wait()

        def build(l, _):
            wn[4 * which + s, l] = side_by_side(raw, raw_s, l, lax.rem(l // dist, 2))
            return 0

        lax.fori_loop(0, LOCAL, build, 0, unroll=4)

    def wa_arrived(slot, sem):
        pltpu.make_async_copy(wa.at[slot, pl.ds(0, 15)], wa.at[slot, pl.ds(0, 15)], sem.at[slot]).wait()

    def wb_arrived(slot, sem):
        pltpu.make_async_copy(wb.at[slot, pl.ds(0, 14)], wb.at[slot, pl.ds(0, 14)], sem.at[slot]).wait()


    in_copy(0).start()
    for s in range(4):
        raw_copy(0, s).start()
    for c in range(1, chunks):
        in_copy(c).start()
    for s in range(4, 11):
        raw_copy(0, s).start()
    for s in range(11):
        raw_copy(1, s).start()


    barrier = pltpu.get_barrier_semaphore()

    def greet(target):
        pl.semaphore_signal(barrier, inc=1, device_id=target, device_id_type=MESH)

    def greet_zy(i, _):
        greet(device(zy ^ i, xc))
        return 0

    def greet_xc(i, _):
        greet(device(zy, xc ^ i))
        return 0

    lax.fori_loop(1, LOCAL, greet_zy, 0)
    lax.fori_loop(1, SUB, greet_xc, 0)
    in_copy(0).wait()
    pl.semaphore_wait(barrier, 15 + 7)

    send_up1(0)
    for s in range(4):
        build_wa(0, s, lax.rem(zy // A_DIST[s], 2))
        send_wa(0, s)
    for c in range(1, AHEAD):
        in_copy(c).wait()
        send_up1(c)
    for s in range(3):
        send_wb(0, s, lax.rem(xc // (B_DIST[s] // 2), 2))
    for s in range(4):
        build_wn(0, s, N_DIST[s])
    for s in range(4):
        build_wn(1, s, N_DIST[3 - s])
    for s in range(3):
        send_wb(1, s, lax.rem(xc // (B_DIST[2 - s] // 2), 2))

    for s in range(3):
        wb_arrived(s, wb_recv)


    def at(c, body):
        pl.when((c >= 0) & (c < chunks))(body)

    def slot_body(t, _):
        def first_a():
            c = t - AT_A1

            @pl.when(c == 0)
            def _():
                for s in range(4):
                    wa_arrived(s, wa_recv)

            arrived(UP1, a1, c)
            run_stages(a1, c, wa, 0, A_DIST)
            send_up2(c)

        at(t - AT_A1, first_a)

        @pl.when(t + AHEAD < chunks)
        def _():
            in_copy(t + AHEAD).wait()
            send_up1(t + AHEAD)

        for s in range(4):

            @pl.when(t == AT_WA2 + s)
            def _(s=s):
                build_wa(1, s, lax.rem(zy // A_DIST[3 - s], 2))
                send_wa(1, s)

        def first_b():
            c = t - AT_B1

            arrived(UP2, b1, c)
            run_stages(b1, c, wb, 0, B_DIST)
            send_up3(c)

        at(t - AT_B1, first_b)

        def middle():
            c = t - AT_N
            arrived(UP3, nb, c)
            run_stages(nb, c, wn, 0, N_DIST, last=gelu)
            run_stages(nb, c, wn, 4, N_DIST[::-1])
            send_down1(c)

        at(t - AT_N, middle)

        def second_b():
            c = t - AT_B2

            @pl.when(c == 0)
            def _():
                for s in range(3):
                    wb_arrived(3 + s, wb_recv)

            arrived(DOWN1, b2, c)
            run_stages(b2, c, wb, 3, B_DIST[::-1])
            send_down2(c)

        at(t - AT_B2, second_b)

        def second_a():
            c = t - AT_A2

            @pl.when(c == 0)
            def _():
                for s in range(4):
                    wa_arrived(4 + s, wa_recv)

            arrived(DOWN2, a2, c)
            run_stages(a2, c, wa, 4, A_DIST[::-1])
            send_down3(c)

        at(t - AT_A2, second_a)

        return 0

    lax.fori_loop(0, chunks + AT_A2, slot_body, 0)

    def finish(c, _):
        drained(UP1, inb, c)
        drained(UP2, a1, c)
        drained(UP3, b1, c)
        drained(DOWN1, nb, c)
        drained(DOWN2, b2, c)
        drained(DOWN3, a2, c)
        own_copy(c).wait()
        return 0

    for slot in range(8):
        wa_arrived(slot, wa_send)
    for slot in range(6):
        wb_arrived(slot, wb_send)
    lax.fori_loop(0, chunks, finish, 0)

    def landed(c, _):
        arrived(DOWN3, ob, c)
        return 0

    lax.fori_loop(0, chunks, landed, 0)


def gather_chunks(chunks, parts, out, buf, in_sem, out_sem):
    into = [pltpu.make_async_copy(parts.at[c], buf.at[c], in_sem.at[c]) for c in range(chunks)]
    onto = [
        pltpu.make_async_copy(buf.at[c], out.at[:, pl.ds(c * LANES, LANES)], out_sem.at[c]) for c in range(chunks)
    ]
    for copy in into:
        copy.start()
    for c in range(chunks):
        into[c].wait()
        onto[c].start()
    for copy in onto:
        copy.wait()


def solution(mesh):
    def device_program(signal, w_first, w_second):
        rows, columns = signal.shape
        stages = w_first.shape[0]
        chunks = columns // LANES
        bf16 = jnp.bfloat16
        moved = pltpu.VMEM((chunks, LOCAL, BLOCK, LANES), bf16)
        raw = pltpu.VMEM((stages, LOCAL, 2, BLOCK, BLOCK), bf16)

        def paired(n):
            return pltpu.VMEM((n, LOCAL, BLOCK, LANES), bf16)

        dma = pltpu.SemaphoreType.DMA
        hbm = pl.BlockSpec(memory_space=pl.ANY)
        result = pl.pallas_call(
            functools.partial(kernel, chunks),
            out_shape=jax.ShapeDtypeStruct((chunks, LOCAL, BLOCK, LANES), bf16),
            in_specs=[hbm, hbm, hbm],
            out_specs=hbm,
            scratch_shapes=[moved] * 6
            + [raw, raw, paired(8), paired(6), paired(8), paired(6), paired(8)]
            + [
                dma((chunks,)),
                dma((2, stages)),
                dma((6, chunks)),
                dma((6, chunks)),
                dma((8,)),
                dma((8,)),
                dma((6,)),
                dma((6,)),
                dma((chunks,)),
            ],
            compiler_params=pltpu.CompilerParams(
                collective_id=0, has_side_effects=True, vmem_limit_bytes=60 * 2**20
            ),
        )(signal.reshape(LOCAL, BLOCK, columns), w_first, w_second)
        return pl.pallas_call(
            functools.partial(gather_chunks, chunks),
            out_shape=jax.ShapeDtypeStruct((rows, columns), bf16),
            in_specs=[hbm],
            out_specs=hbm,
            scratch_shapes=[pltpu.VMEM((chunks, rows, LANES), bf16), dma((chunks,)), dma((chunks,))],
            compiler_params=pltpu.CompilerParams(vmem_limit_bytes=60 * 2**20),
        )(result.reshape(chunks, rows, LANES))

    row_spec = P(("dp", "sp"), None)
    weight_spec = P(None, "sp", None, None, None)
    return jax.shard_map(
        device_program, mesh=mesh, in_specs=(row_spec, weight_spec, weight_spec), out_specs=row_spec, check_vma=False
    )
```

```python
import functools

import jax
import jax.numpy as jnp
from jax import lax
from jax.experimental import pallas as pl
from jax.experimental.pallas import tpu as pltpu
from jax.sharding import PartitionSpec as P

MESH = pl.DeviceIdType.MESH

LANES = 128
BLOCK = 64
HALF = 32
LOCAL = 16
SUB = 8
A_DIST = (8, 4, 2, 1)
B_DIST = (8, 4, 2)
N_DIST = (8, 4, 2, 1)
UP1, UP2, UP3, DOWN1, DOWN2, DOWN3 = range(6)
AT_A1, AT_B1, AT_N, AT_B2, AT_A2 = 0, 2, 4, 6, 8
AHEAD = 3
AT_WA2 = 3


def swap(v):
    return lax.rem(v, 2) + 2 * (v // 4) + 4 * lax.rem(v // 2, 2)


def spread(i):
    return (15 * lax.rem(i, 2)) ^ (5 * lax.rem(i // 2, 2)) ^ (3 * lax.rem(i // 4, 2)) ^ (i // 8)


def gelu(x):
    return 0.5 * x * (1.0 + lax.erf(x * (0.5**0.5)))


def run_stages(buf, c, weights, stage0, dists, last=None):
    for step, dist in enumerate(dists):
        for low in range(LOCAL):
            if low & dist:
                continue
            high = low + dist
            act = jnp.concatenate([buf[c, low], buf[c, high]], axis=0)
            mat = jnp.concatenate([weights[stage0 + step, low], weights[stage0 + step, high]], axis=0)
            mixed = jnp.dot(mat, act, preferred_element_type=jnp.float32)
            if last is not None and step == len(dists) - 1:
                mixed = last(mixed.astype(jnp.bfloat16).astype(jnp.float32))
            mixed = mixed.astype(jnp.bfloat16)
            buf[c, low] = mixed[:BLOCK]
            buf[c, high] = mixed[BLOCK:]


def kernel(
    chunks,
    sig, w1, w2, ob,
    inb, a1, b1, nb, b2, a2,
    raw1, raw2, send_a, send_b, wa, wb, wn,
    in_sem, raw_sem, move_send, move_recv, wa_send, wa_recv, wb_send, wb_recv, out_sem,
):
    me = lax.axis_index("sp")
    zy = me // SUB
    xc = lax.rem(me, SUB)
    twist = 2 * swap(xc ^ 7)
    half = zy // 2
    own_l = zy ^ twist
    own_h = swap(xc) ^ half

    def device(zy_, xc_):
        return {"sp": zy_ * SUB + xc_}

    def remote(src, dst, send, recv, target):
        return pltpu.make_async_remote_copy(
            src_ref=src, dst_ref=dst, send_sem=send, recv_sem=recv, device_id=target, device_id_type=MESH
        )

    def in_copy(c):
        return pltpu.make_async_copy(sig.at[:, :, pl.ds(c * LANES, LANES)], inb.at[c], in_sem.at[c])

    def raw_copy(which, s):
        src, dst = ((w1, raw1), (w2, raw2))[which]
        return pltpu.make_async_copy(src.at[s], dst.at[s], raw_sem.at[which, s])

    def own_copy(c):
        return pltpu.make_async_copy(a2.at[c, zy], ob.at[c, own_l], out_sem.at[c])


    def send_up1(c):
        def one(i, _):
            to = zy ^ (1 + lax.rem(i, LOCAL - 1))
            rows = pl.ds((i // (LOCAL - 1)) * HALF, HALF)
            remote(
                inb.at[c, to ^ twist, rows], a1.at[c, zy, rows], move_send.at[UP1, c], move_recv.at[UP1, c],
                device(to, xc),
            ).start()
            return 0

        lax.fori_loop(0, 2 * (LOCAL - 1), one, 0, unroll=6)
        a1[c, zy] = inb[c, own_l]

    def send_up2(c):
        def one(i, _):
            q = zy ^ spread(lax.rem(i, LOCAL))
            rows = pl.ds((i // LOCAL) * HALF, HALF)
            remote(
                a1.at[c, q, rows], b1.at[c, 2 * xc + lax.rem(own_l, 2), rows], move_send.at[UP2, c],
                move_recv.at[UP2, c], device(q, swap((own_l // 2) ^ (q // 2))),
            ).start()
            return 0

        lax.fori_loop(0, 2 * LOCAL, one, 0, unroll=8)

    def send_up3(c):
        def one(i, _):
            t = xc ^ i
            remote(
                b1.at[c, pl.ds(2 * t, 2)], nb.at[c, pl.ds(2 * own_h, 2)], move_send.at[UP3, c], move_recv.at[UP3, c],
                device(zy, t),
            ).start()
            return 0

        lax.fori_loop(1, SUB, one, 0, unroll=7)
        nb[c, pl.ds(2 * own_h, 2)] = b1[c, pl.ds(2 * xc, 2)]

    def send_down1(c):
        def one(i, _):
            to = xc ^ i
            remote(
                nb.at[c, pl.ds(2 * (swap(to) ^ half), 2)], b2.at[c, pl.ds(2 * xc, 2)], move_send.at[DOWN1, c],
                move_recv.at[DOWN1, c], device(zy, to),
            ).start()
            return 0

        lax.fori_loop(1, SUB, one, 0, unroll=7)
        b2[c, pl.ds(2 * xc, 2)] = nb[c, pl.ds(2 * own_h, 2)]

    def send_down2(c):
        def one(i, _):
            step = spread(lax.rem(i, LOCAL))
            to, t = zy ^ step, xc ^ swap(step // 2) ^ 7
            rows = pl.ds((i // LOCAL) * HALF, HALF)
            remote(
                b2.at[c, 2 * t + lax.rem(to, 2), rows], a2.at[c, zy, rows], move_send.at[DOWN2, c],
                move_recv.at[DOWN2, c], device(to, t),
            ).start()
            return 0

        lax.fori_loop(0, 2 * LOCAL, one, 0, unroll=8)

    def send_down3(c):
        def one(i, _):
            q = zy ^ (1 + lax.rem(i, LOCAL - 1))
            rows = pl.ds((i // (LOCAL - 1)) * HALF, HALF)
            remote(
                a2.at[c, q, rows], ob.at[c, own_l, rows], move_send.at[DOWN3, c], move_recv.at[DOWN3, c],
                device(q, xc),
            ).start()
            return 0

        lax.fori_loop(0, 2 * (LOCAL - 1), one, 0, unroll=6)
        own_copy(c).start()

    remote_blocks = {UP1: 15, UP2: 16, UP3: 14, DOWN1: 14, DOWN2: 16, DOWN3: 15}

    def arrived(move, buf, c):
        n = remote_blocks[move]
        pltpu.make_async_copy(buf.at[c, pl.ds(0, n)], buf.at[c, pl.ds(0, n)], move_recv.at[move, c]).wait()

    def drained(move, buf, c):
        n = remote_blocks[move]
        pltpu.make_async_copy(buf.at[c, pl.ds(0, n)], buf.at[c, pl.ds(0, n)], move_send.at[move, c]).wait()


    def side_by_side(raw, s, l, bit):
        return jnp.concatenate([raw[s, l, bit], raw[s, l, 1 - bit]], axis=1)

    def build_wa(which, s, bit):
        raw = (raw1, raw2)[which]
        raw_s = s if which == 0 else 7 + s
        raw_copy(which, raw_s).wait()
        slot = 4 * which + s

        def build(l, _):
            send_a[slot, l] = side_by_side(raw, raw_s, l, bit)
            return 0

        lax.fori_loop(0, LOCAL, build, 0, unroll=4)

    def send_wa(which, s):
        slot = 4 * which + s

        def one(i, _):
            to = zy ^ (1 + lax.rem(i, LOCAL - 1))
            rows = pl.ds((i // (LOCAL - 1)) * HALF, HALF)
            remote(
                send_a.at[slot, to ^ twist, rows], wa.at[slot, zy, rows], wa_send.at[slot], wa_recv.at[slot],
                device(to, xc),
            ).start()
            return 0

        lax.fori_loop(0, 2 * (LOCAL - 1), one, 0, unroll=6)
        wa[slot, zy] = send_a[slot, own_l]

    def send_wb(which, s, bit):
        raw = (raw1, raw2)[which]
        raw_copy(which, 4 + s).wait()
        slot = 3 * which + s

        def build(l, _):
            send_b[slot, l] = side_by_side(raw, 4 + s, l, bit)
            return 0

        lax.fori_loop(0, LOCAL, build, 0, unroll=4)

        def one(i, _):
            to = xc ^ i
            remote(
                send_b.at[slot, pl.ds(2 * (swap(to) ^ half), 2)], wb.at[slot, pl.ds(2 * xc, 2)], wb_send.at[slot],
                wb_recv.at[slot], device(zy, to),
            ).start()
            return 0

        lax.fori_loop(1, SUB, one, 0, unroll=7)
        wb[slot, pl.ds(2 * xc, 2)] = send_b[slot, pl.ds(2 * own_h, 2)]

    def build_wn(which, s, dist):
        raw = (raw1, raw2)[which]
        raw_s = 7 + s if which == 0 else s
        raw_copy(which, raw_s).wait()

        def build(l, _):
            wn[4 * which + s, l] = side_by_side(raw, raw_s, l, lax.rem(l // dist, 2))
            return 0

        lax.fori_loop(0, LOCAL, build, 0, unroll=4)

    def wa_arrived(slot, sem):
        pltpu.make_async_copy(wa.at[slot, pl.ds(0, 15)], wa.at[slot, pl.ds(0, 15)], sem.at[slot]).wait()

    def wb_arrived(slot, sem):
        pltpu.make_async_copy(wb.at[slot, pl.ds(0, 14)], wb.at[slot, pl.ds(0, 14)], sem.at[slot]).wait()


    in_copy(0).start()
    for s in range(4):
        raw_copy(0, s).start()
    for c in range(1, chunks):
        in_copy(c).start()
    for s in range(4, 11):
        raw_copy(0, s).start()
    for s in range(11):
        raw_copy(1, s).start()


    barrier = pltpu.get_barrier_semaphore()

    def greet(target):
        pl.semaphore_signal(barrier, inc=1, device_id=target, device_id_type=MESH)

    def greet_zy(i, _):
        greet(device(zy ^ i, xc))
        return 0

    def greet_xc(i, _):
        greet(device(zy, xc ^ i))
        return 0

    lax.fori_loop(1, LOCAL, greet_zy, 0)
    lax.fori_loop(1, SUB, greet_xc, 0)
    in_copy(0).wait()
    pl.semaphore_wait(barrier, 15 + 7)

    send_up1(0)
    for s in range(4):
        build_wa(0, s, lax.rem(zy // A_DIST[s], 2))
        send_wa(0, s)
    for c in range(1, AHEAD):
        in_copy(c).wait()
        send_up1(c)
    for s in range(3):
        send_wb(0, s, lax.rem(xc // (B_DIST[s] // 2), 2))
    for s in range(4):
        build_wn(0, s, N_DIST[s])
    for s in range(4):
        build_wn(1, s, N_DIST[3 - s])
    for s in range(3):
        send_wb(1, s, lax.rem(xc // (B_DIST[2 - s] // 2), 2))

    for s in range(3):
        wb_arrived(s, wb_recv)


    def at(c, body):
        pl.when((c >= 0) & (c < chunks))(body)

    def slot_body(t, _):
        def first_a():
            c = t - AT_A1

            @pl.when(c == 0)
            def _():
                for s in range(4):
                    wa_arrived(s, wa_recv)

            arrived(UP1, a1, c)
            run_stages(a1, c, wa, 0, A_DIST)
            send_up2(c)

        at(t - AT_A1, first_a)

        @pl.when(t + AHEAD < chunks)
        def _():
            in_copy(t + AHEAD).wait()
            send_up1(t + AHEAD)

        for s in range(4):

            @pl.when(t == AT_WA2 + s)
            def _(s=s):
                build_wa(1, s, lax.rem(zy // A_DIST[3 - s], 2))
                send_wa(1, s)

        def first_b():
            c = t - AT_B1

            arrived(UP2, b1, c)
            run_stages(b1, c, wb, 0, B_DIST)
            send_up3(c)

        at(t - AT_B1, first_b)

        def middle():
            c = t - AT_N
            arrived(UP3, nb, c)
            run_stages(nb, c, wn, 0, N_DIST, last=gelu)
            run_stages(nb, c, wn, 4, N_DIST[::-1])
            send_down1(c)

        at(t - AT_N, middle)

        def second_b():
            c = t - AT_B2

            @pl.when(c == 0)
            def _():
                for s in range(3):
                    wb_arrived(3 + s, wb_recv)

            arrived(DOWN1, b2, c)
            run_stages(b2, c, wb, 3, B_DIST[::-1])
            send_down2(c)

        at(t - AT_B2, second_b)

        def second_a():
            c = t - AT_A2

            @pl.when(c == 0)
            def _():
                for s in range(4):
                    wa_arrived(4 + s, wa_recv)

            arrived(DOWN2, a2, c)
            run_stages(a2, c, wa, 4, A_DIST[::-1])
            send_down3(c)

        at(t - AT_A2, second_a)

        return 0

    lax.fori_loop(0, chunks + AT_A2, slot_body, 0)

    def finish(c, _):
        drained(UP1, inb, c)
        drained(UP2, a1, c)
        drained(UP3, b1, c)
        drained(DOWN1, nb, c)
        drained(DOWN2, b2, c)
        drained(DOWN3, a2, c)
        own_copy(c).wait()
        return 0

    for slot in range(8):
        wa_arrived(slot, wa_send)
    for slot in range(6):
        wb_arrived(slot, wb_send)
    lax.fori_loop(0, chunks, finish, 0)

    def landed(c, _):
        arrived(DOWN3, ob, c)
        return 0

    lax.fori_loop(0, chunks, landed, 0)


def gather_chunks(chunks, parts, out, buf, in_sem, out_sem):
    into = [pltpu.make_async_copy(parts.at[c], buf.at[c], in_sem.at[c]) for c in range(chunks)]
    onto = [
        pltpu.make_async_copy(buf.at[c], out.at[:, pl.ds(c * LANES, LANES)], out_sem.at[c]) for c in range(chunks)
    ]
    for copy in into:
        copy.start()
    for c in range(chunks):
        into[c].wait()
        onto[c].start()
    for copy in onto:
        copy.wait()


def solution(mesh):
    def device_program(signal, w_first, w_second):
        rows, columns = signal.shape
        stages = w_first.shape[0]
        chunks = columns // LANES
        bf16 = jnp.bfloat16
        moved = pltpu.VMEM((chunks, LOCAL, BLOCK, LANES), bf16)
        raw = pltpu.VMEM((stages, LOCAL, 2, BLOCK, BLOCK), bf16)

        def paired(n):
            return pltpu.VMEM((n, LOCAL, BLOCK, LANES), bf16)

        dma = pltpu.SemaphoreType.DMA
        hbm = pl.BlockSpec(memory_space=pl.ANY)
        result = pl.pallas_call(
            functools.partial(kernel, chunks),
            out_shape=jax.ShapeDtypeStruct((chunks, LOCAL, BLOCK, LANES), bf16),
            in_specs=[hbm, hbm, hbm],
            out_specs=hbm,
            scratch_shapes=[moved] * 6
            + [raw, raw, paired(8), paired(6), paired(8), paired(6), paired(8)]
            + [
                dma((chunks,)),
                dma((2, stages)),
                dma((6, chunks)),
                dma((6, chunks)),
                dma((8,)),
                dma((8,)),
                dma((6,)),
                dma((6,)),
                dma((chunks,)),
            ],
            compiler_params=pltpu.CompilerParams(
                collective_id=0, has_side_effects=True, vmem_limit_bytes=60 * 2**20
            ),
        )(signal.reshape(LOCAL, BLOCK, columns), w_first, w_second)
        return pl.pallas_call(
            functools.partial(gather_chunks, chunks),
            out_shape=jax.ShapeDtypeStruct((rows, columns), bf16),
            in_specs=[hbm],
            out_specs=hbm,
            scratch_shapes=[pltpu.VMEM((chunks, rows, LANES), bf16), dma((chunks,)), dma((chunks,))],
            compiler_params=pltpu.CompilerParams(vmem_limit_bytes=60 * 2**20),
        )(result.reshape(chunks, rows, LANES))

    row_spec = P(("dp", "sp"), None)
    weight_spec = P(None, "sp", None, None, None)
    return jax.shard_map(
        device_program, mesh=mesh, in_specs=(row_spec, weight_spec, weight_spec), out_specs=row_spec, check_vma=False
    )
```

```python
import functools

import jax
import jax.numpy as jnp
from jax import lax
from jax.experimental import pallas as pl
from jax.experimental.pallas import tpu as pltpu
from jax.sharding import PartitionSpec as P

MESH = pl.DeviceIdType.MESH

LANES = 128
BLOCK = 64
HALF = 32
LOCAL = 16
SUB = 8
A_DIST = (8, 4, 2, 1)
B_DIST = (8, 4, 2)
N_DIST = (8, 4, 2, 1)
UP1, UP2, UP3, DOWN1, DOWN2, DOWN3 = range(6)
AT_A1, AT_B1, AT_N, AT_B2, AT_A2 = 0, 2, 4, 6, 8
AHEAD = 3
AT_WA2 = 3


def swap(v):
    return lax.rem(v, 2) + 2 * (v // 4) + 4 * lax.rem(v // 2, 2)


def spread(i):
    return (15 * lax.rem(i, 2)) ^ (5 * lax.rem(i // 2, 2)) ^ (3 * lax.rem(i // 4, 2)) ^ (i // 8)


def gelu(x):
    return 0.5 * x * (1.0 + lax.erf(x * (0.5**0.5)))


def run_stages(buf, c, weights, stage0, dists, last=None):
    for step, dist in enumerate(dists):
        for low in range(LOCAL):
            if low & dist:
                continue
            high = low + dist
            act = jnp.concatenate([buf[c, low], buf[c, high]], axis=0)
            mat = jnp.concatenate([weights[stage0 + step, low], weights[stage0 + step, high]], axis=0)
            mixed = jnp.dot(mat, act, preferred_element_type=jnp.float32)
            if last is not None and step == len(dists) - 1:
                mixed = last(mixed.astype(jnp.bfloat16).astype(jnp.float32))
            mixed = mixed.astype(jnp.bfloat16)
            buf[c, low] = mixed[:BLOCK]
            buf[c, high] = mixed[BLOCK:]


def kernel(
    chunks,
    sig, w1, w2, ob,
    inb, a1, b1, nb, b2, a2,
    raw1, raw2, send_a, send_b, wa, wb, wn,
    in_sem, raw_sem, move_send, move_recv, wa_send, wa_recv, wb_send, wb_recv, out_sem,
):
    me = lax.axis_index("sp")
    zy = me // SUB
    xc = lax.rem(me, SUB)
    twist = 2 * swap(xc ^ 7)
    half = zy // 2
    own_l = zy ^ twist
    own_h = swap(xc) ^ half

    def device(zy_, xc_):
        return {"sp": zy_ * SUB + xc_}

    def remote(src, dst, send, recv, target):
        return pltpu.make_async_remote_copy(
            src_ref=src, dst_ref=dst, send_sem=send, recv_sem=recv, device_id=target, device_id_type=MESH
        )

    def in_copy(c):
        return pltpu.make_async_copy(sig.at[:, :, pl.ds(c * LANES, LANES)], inb.at[c], in_sem.at[c])

    def raw_copy(which, s):
        src, dst = ((w1, raw1), (w2, raw2))[which]
        return pltpu.make_async_copy(src.at[s], dst.at[s], raw_sem.at[which, s])

    def own_copy(c):
        return pltpu.make_async_copy(a2.at[c, zy], ob.at[c, own_l], out_sem.at[c])


    def send_up1(c):
        def one(i, _):
            to = zy ^ (1 + lax.rem(i, LOCAL - 1))
            rows = pl.ds((i // (LOCAL - 1)) * HALF, HALF)
            remote(
                inb.at[c, to ^ twist, rows], a1.at[c, zy, rows], move_send.at[UP1, c], move_recv.at[UP1, c],
                device(to, xc),
            ).start()
            return 0

        lax.fori_loop(0, 2 * (LOCAL - 1), one, 0, unroll=6)
        a1[c, zy] = inb[c, own_l]

    def send_up2(c):
        def one(i, _):
            q = zy ^ spread(lax.rem(i, LOCAL))
            rows = pl.ds((i // LOCAL) * HALF, HALF)
            remote(
                a1.at[c, q, rows], b1.at[c, 2 * xc + lax.rem(own_l, 2), rows], move_send.at[UP2, c],
                move_recv.at[UP2, c], device(q, swap((own_l // 2) ^ (q // 2))),
            ).start()
            return 0

        lax.fori_loop(0, 2 * LOCAL, one, 0, unroll=8)

    def send_up3(c):
        def one(i, _):
            t = xc ^ i
            remote(
                b1.at[c, pl.ds(2 * t, 2)], nb.at[c, pl.ds(2 * own_h, 2)], move_send.at[UP3, c], move_recv.at[UP3, c],
                device(zy, t),
            ).start()
            return 0

        lax.fori_loop(1, SUB, one, 0, unroll=7)
        nb[c, pl.ds(2 * own_h, 2)] = b1[c, pl.ds(2 * xc, 2)]

    def send_down1(c):
        def one(i, _):
            to = xc ^ i
            remote(
                nb.at[c, pl.ds(2 * (swap(to) ^ half), 2)], b2.at[c, pl.ds(2 * xc, 2)], move_send.at[DOWN1, c],
                move_recv.at[DOWN1, c], device(zy, to),
            ).start()
            return 0

        lax.fori_loop(1, SUB, one, 0, unroll=7)
        b2[c, pl.ds(2 * xc, 2)] = nb[c, pl.ds(2 * own_h, 2)]

    def send_down2(c):
        def one(i, _):
            step = spread(lax.rem(i, LOCAL))
            to, t = zy ^ step, xc ^ swap(step // 2) ^ 7
            rows = pl.ds((i // LOCAL) * HALF, HALF)
            remote(
                b2.at[c, 2 * t + lax.rem(to, 2), rows], a2.at[c, zy, rows], move_send.at[DOWN2, c],
                move_recv.at[DOWN2, c], device(to, t),
            ).start()
            return 0

        lax.fori_loop(0, 2 * LOCAL, one, 0, unroll=8)

    def send_down3(c):
        def one(i, _):
            q = zy ^ (1 + lax.rem(i, LOCAL - 1))
            rows = pl.ds((i // (LOCAL - 1)) * HALF, HALF)
            remote(
                a2.at[c, q, rows], ob.at[c, own_l, rows], move_send.at[DOWN3, c], move_recv.at[DOWN3, c],
                device(q, xc),
            ).start()
            return 0

        lax.fori_loop(0, 2 * (LOCAL - 1), one, 0, unroll=6)
        own_copy(c).start()

    remote_blocks = {UP1: 15, UP2: 16, UP3: 14, DOWN1: 14, DOWN2: 16, DOWN3: 15}

    def arrived(move, buf, c):
        n = remote_blocks[move]
        pltpu.make_async_copy(buf.at[c, pl.ds(0, n)], buf.at[c, pl.ds(0, n)], move_recv.at[move, c]).wait()

    def drained(move, buf, c):
        n = remote_blocks[move]
        pltpu.make_async_copy(buf.at[c, pl.ds(0, n)], buf.at[c, pl.ds(0, n)], move_send.at[move, c]).wait()


    def side_by_side(raw, s, l, bit):
        return jnp.concatenate([raw[s, l, bit], raw[s, l, 1 - bit]], axis=1)

    def build_wa(which, s, bit):
        raw = (raw1, raw2)[which]
        raw_s = s if which == 0 else 7 + s
        raw_copy(which, raw_s).wait()
        slot = 4 * which + s

        def build(l, _):
            send_a[slot, l] = side_by_side(raw, raw_s, l, bit)
            return 0

        lax.fori_loop(0, LOCAL, build, 0, unroll=4)

    def send_wa(which, s):
        slot = 4 * which + s

        def one(i, _):
            to = zy ^ (1 + lax.rem(i, LOCAL - 1))
            rows = pl.ds((i // (LOCAL - 1)) * HALF, HALF)
            remote(
                send_a.at[slot, to ^ twist, rows], wa.at[slot, zy, rows], wa_send.at[slot], wa_recv.at[slot],
                device(to, xc),
            ).start()
            return 0

        lax.fori_loop(0, 2 * (LOCAL - 1), one, 0, unroll=6)
        wa[slot, zy] = send_a[slot, own_l]

    def send_wb(which, s, bit):
        raw = (raw1, raw2)[which]
        raw_copy(which, 4 + s).wait()
        slot = 3 * which + s

        def build(l, _):
            send_b[slot, l] = side_by_side(raw, 4 + s, l, bit)
            return 0

        lax.fori_loop(0, LOCAL, build, 0, unroll=4)

        def one(i, _):
            to = xc ^ i
            remote(
                send_b.at[slot, pl.ds(2 * (swap(to) ^ half), 2)], wb.at[slot, pl.ds(2 * xc, 2)], wb_send.at[slot],
                wb_recv.at[slot], device(zy, to),
            ).start()
            return 0

        lax.fori_loop(1, SUB, one, 0, unroll=7)
        wb[slot, pl.ds(2 * xc, 2)] = send_b[slot, pl.ds(2 * own_h, 2)]

    def build_wn(which, s, dist):
        raw = (raw1, raw2)[which]
        raw_s = 7 + s if which == 0 else s
        raw_copy(which, raw_s).wait()

        def build(l, _):
            wn[4 * which + s, l] = side_by_side(raw, raw_s, l, lax.rem(l // dist, 2))
            return 0

        lax.fori_loop(0, LOCAL, build, 0, unroll=4)

    def wa_arrived(slot, sem):
        pltpu.make_async_copy(wa.at[slot, pl.ds(0, 15)], wa.at[slot, pl.ds(0, 15)], sem.at[slot]).wait()

    def wb_arrived(slot, sem):
        pltpu.make_async_copy(wb.at[slot, pl.ds(0, 14)], wb.at[slot, pl.ds(0, 14)], sem.at[slot]).wait()


    in_copy(0).start()
    for s in range(7):
        raw_copy(0, s).start()
    for s in range(4, 7):
        raw_copy(1, s).start()
    for c in range(1, chunks):
        in_copy(c).start()
    for s in range(7, 11):
        raw_copy(0, s).start()
    for s in (0, 1, 2, 3, 7, 8, 9, 10):
        raw_copy(1, s).start()


    barrier = pltpu.get_barrier_semaphore()

    def greet(target):
        pl.semaphore_signal(barrier, inc=1, device_id=target, device_id_type=MESH)

    def greet_zy(i, _):
        greet(device(zy ^ i, xc))
        return 0

    def greet_xc(i, _):
        greet(device(zy, xc ^ i))
        return 0

    lax.fori_loop(1, LOCAL, greet_zy, 0)
    lax.fori_loop(1, SUB, greet_xc, 0)
    in_copy(0).wait()
    pl.semaphore_wait(barrier, 15 + 7)

    send_up1(0)
    for s in range(4):
        build_wa(0, s, lax.rem(zy // A_DIST[s], 2))
        send_wa(0, s)
        if s < 3:
            send_wb(0, s, lax.rem(xc // (B_DIST[s] // 2), 2))
    for s in range(3):
        send_wb(1, s, lax.rem(xc // (B_DIST[2 - s] // 2), 2))
    for c in range(1, AHEAD):
        in_copy(c).wait()
        send_up1(c)
    for s in range(4):
        build_wn(0, s, N_DIST[s])
    for s in range(4):
        build_wn(1, s, N_DIST[3 - s])

    for s in range(3):
        wb_arrived(s, wb_recv)


    def at(c, body):
        pl.when((c >= 0) & (c < chunks))(body)

    def slot_body(t, _):
        def first_a():
            c = t - AT_A1

            arrived(UP1, a1, c)

            @pl.when(c == 0)
            def _():
                for s in range(4):
                    wa_arrived(s, wa_recv)
                    run_stages(a1, c, wa, s, (A_DIST[s],))

            @pl.when(c > 0)
            def _():
                run_stages(a1, c, wa, 0, A_DIST)

            send_up2(c)

        at(t - AT_A1, first_a)

        @pl.when(t + AHEAD < chunks)
        def _():
            in_copy(t + AHEAD).wait()
            send_up1(t + AHEAD)

        for s in range(4):

            @pl.when(t == AT_WA2 + s)
            def _(s=s):
                build_wa(1, s, lax.rem(zy // A_DIST[3 - s], 2))
                send_wa(1, s)

        def first_b():
            c = t - AT_B1

            arrived(UP2, b1, c)
            run_stages(b1, c, wb, 0, B_DIST)
            send_up3(c)

        at(t - AT_B1, first_b)

        def middle():
            c = t - AT_N
            arrived(UP3, nb, c)
            run_stages(nb, c, wn, 0, N_DIST, last=gelu)
            run_stages(nb, c, wn, 4, N_DIST[::-1])
            send_down1(c)

        at(t - AT_N, middle)

        def second_b():
            c = t - AT_B2

            @pl.when(c == 0)
            def _():
                for s in range(3):
                    wb_arrived(3 + s, wb_recv)

            arrived(DOWN1, b2, c)
            run_stages(b2, c, wb, 3, B_DIST[::-1])
            send_down2(c)

        at(t - AT_B2, second_b)

        def second_a():
            c = t - AT_A2

            @pl.when(c == 0)
            def _():
                for s in range(4):
                    wa_arrived(4 + s, wa_recv)

            arrived(DOWN2, a2, c)
            run_stages(a2, c, wa, 4, A_DIST[::-1])
            send_down3(c)

        at(t - AT_A2, second_a)

        return 0

    lax.fori_loop(0, chunks + AT_A2, slot_body, 0)

    def finish(c, _):
        drained(UP1, inb, c)
        drained(UP2, a1, c)
        drained(UP3, b1, c)
        drained(DOWN1, nb, c)
        drained(DOWN2, b2, c)
        drained(DOWN3, a2, c)
        own_copy(c).wait()
        return 0

    for slot in range(8):
        wa_arrived(slot, wa_send)
    for slot in range(6):
        wb_arrived(slot, wb_send)
    lax.fori_loop(0, chunks, finish, 0)

    def landed(c, _):
        arrived(DOWN3, ob, c)
        return 0

    lax.fori_loop(0, chunks, landed, 0)


def gather_chunks(chunks, parts, out, buf, in_sem, out_sem):
    into = [pltpu.make_async_copy(parts.at[c], buf.at[c], in_sem.at[c]) for c in range(chunks)]
    onto = [
        pltpu.make_async_copy(buf.at[c], out.at[:, pl.ds(c * LANES, LANES)], out_sem.at[c]) for c in range(chunks)
    ]
    for copy in into:
        copy.start()
    for c in range(chunks):
        into[c].wait()
        onto[c].start()
    for copy in onto:
        copy.wait()


def solution(mesh):
    def device_program(signal, w_first, w_second):
        rows, columns = signal.shape
        stages = w_first.shape[0]
        chunks = columns // LANES
        bf16 = jnp.bfloat16
        moved = pltpu.VMEM((chunks, LOCAL, BLOCK, LANES), bf16)
        raw = pltpu.VMEM((stages, LOCAL, 2, BLOCK, BLOCK), bf16)

        def paired(n):
            return pltpu.VMEM((n, LOCAL, BLOCK, LANES), bf16)

        dma = pltpu.SemaphoreType.DMA
        hbm = pl.BlockSpec(memory_space=pl.ANY)
        result = pl.pallas_call(
            functools.partial(kernel, chunks),
            out_shape=jax.ShapeDtypeStruct((chunks, LOCAL, BLOCK, LANES), bf16),
            in_specs=[hbm, hbm, hbm],
            out_specs=hbm,
            scratch_shapes=[moved] * 6
            + [raw, raw, paired(8), paired(6), paired(8), paired(6), paired(8)]
            + [
                dma((chunks,)),
                dma((2, stages)),
                dma((6, chunks)),
                dma((6, chunks)),
                dma((8,)),
                dma((8,)),
                dma((6,)),
                dma((6,)),
                dma((chunks,)),
            ],
            compiler_params=pltpu.CompilerParams(
                collective_id=0, has_side_effects=True, vmem_limit_bytes=60 * 2**20
            ),
        )(signal.reshape(LOCAL, BLOCK, columns), w_first, w_second)
        return pl.pallas_call(
            functools.partial(gather_chunks, chunks),
            out_shape=jax.ShapeDtypeStruct((rows, columns), bf16),
            in_specs=[hbm],
            out_specs=hbm,
            scratch_shapes=[pltpu.VMEM((chunks, rows, LANES), bf16), dma((chunks,)), dma((chunks,))],
            compiler_params=pltpu.CompilerParams(vmem_limit_bytes=60 * 2**20),
        )(result.reshape(chunks, rows, LANES))

    row_spec = P(("dp", "sp"), None)
    weight_spec = P(None, "sp", None, None, None)
    return jax.shard_map(
        device_program, mesh=mesh, in_specs=(row_spec, weight_spec, weight_spec), out_specs=row_spec, check_vma=False
    )
```
